32 devices in a mesh: dp: 4 (over x, core), vocab: 8 (over z, y).
Axes of the slice: x: 2, y: 2, z: 4, core: 2. Of those that a mesh axis runs over, the one named last changes fastest.
Arguments:
- hidden: bfloat16 [256, 4608], P(('dp', 'vocab')), may hold values from -6 to 6
- embedding: bfloat16 [4096, 4608], P('vocab'), may hold values from -0.25 to 0.25
- targets: int32 [256], P('dp'), may hold values from 0 to 4095
- grammar_bits: int32 [256, 128], P('dp', 'vocab'), may hold values from -2147483648 to 2147483647, as said below
Outputs:
- token_loss: float32 [256], P('dp')
- hidden_grad: float32 [256, 4608], P(('dp', 'vocab'))
- embed_grad: float32 [4096, 4608], P('vocab', 'dp')
The draws below stay inside these ranges and needn't reach their ends.
Inputs may be any that keep to these rules, and one draw needn't show every extreme that they name: `grammar_bits`: bit b of word k of a token's row stands for vocabulary entry 32 k + b. Each 128-entry block of a row is either drawn at random or all zero, with a share of zero blocks that differs from block to block of the vocabulary.
All inputs are finite; a program needn't handle non-finite values.
Results may differ from the reference program's by a relative error of at most 0.0023.
Values may be sent and summed in bfloat16 or wider, within the bound.
A program may use at most 128 MiB of HBM per device.

```python
import math
import jax
import jax.numpy as jnp
import numpy as np
from jax import lax

D = 4608
VOCAB = 4096
TOKENS = 256


def draw_grammar_bits(key, part):
    word_count = VOCAB // 32
    key_list = jax.random.split(jax.random.fold_in(key, 17), 4)
    upper_half = jax.random.randint(key_list[0], (TOKENS, word_count), 0, 65536, dtype=jnp.int32)
    lower_half = jax.random.randint(key_list[1], (TOKENS, word_count), 0, 65536, dtype=jnp.int32)
    packed = (upper_half - 32768) * 65536 + lower_half
    block_level = jax.random.randint(key_list[2], (1, VOCAB // 128), 10, 90, dtype=jnp.int32)
    block_roll = jax.random.randint(key_list[3], (TOKENS, VOCAB // 128), 0, 100, dtype=jnp.int32)
    block_keep = (block_roll < block_level).astype(jnp.int32)
    block_keep = jnp.repeat(block_keep, 4, axis=1)
    return packed * block_keep


def touch_ends(result, stream_key, smallest, top_value):
    extent = result.shape
    place = [jax.random.randint(jax.random.fold_in(stream_key, axis), (), 0, extent[axis]) for axis in range(len(extent))]
    result = result.at[tuple(place)].set(smallest)
    longest = extent.index(max(extent))
    place[longest] = (place[longest] + 1) % extent[longest]
    return result.at[tuple(place)].set(top_value)


def block_scale(rng, shape, cuts, smallest, high):
    def one(dim, shards_of):
        draws = jax.random.uniform(jax.random.fold_in(jax.random.fold_in(rng, 6), dim), (shards_of,), jnp.float32, smallest / len(cuts), high / len(cuts))
        return jnp.repeat(jnp.exp(draws), shape[dim] // shards_of).reshape((-1,) + (1,) * (len(shape) - dim - 1))

    level = one(*cuts[0])
    for cut in cuts[1:]:
        level = level * one(*cut)
    return level


def cumulative_ranks(number_of, slope):
    portions = [(1 << 20) // math.isqrt(grade ** slope) + 1 for grade in range(1, number_of + 1)]
    width = 1 + sum(portions) // (1 << 30)
    return np.cumsum(np.array([max(1, weight // width) for weight in portions]))


def skewed_ids(key, shape, number_of, slope):
    listing = cumulative_ranks(number_of, slope)
    pick = jax.random.randint(jax.random.fold_in(key, 1), shape, 0, int(listing[number_of - 1]))
    grade = jnp.searchsorted(jnp.asarray(listing, jnp.int32), pick, side="right")
    return jax.random.permutation(jax.random.fold_in(key, 2), number_of)[grade].astype(jnp.int32)


def normal_values(stream_key, shape, deviation, bound, cuts=(), kind=jnp.bfloat16):
    level = block_scale(stream_key, shape, cuts, -0.22, 0.18) if cuts else 1.0
    result = jax.random.normal(stream_key, shape, jnp.float32) * deviation * level
    return jnp.minimum(jnp.maximum(result, -bound), bound).astype(kind)


def setup_inputs(seed: int = 0) -> dict:
    splits = jax.random.split(jax.random.key(seed), 5)
    return {
        "hidden": normal_values(splits[0], (TOKENS, D), 1.0, 6.0, ((0, 32),)),
        "embedding": normal_values(splits[1], (VOCAB, D), (D // 9) ** -0.5, 0.25, ((0, 8),)),
        "targets": touch_ends(skewed_ids(splits[2], (TOKENS,), VOCAB, 2), jax.random.fold_in(splits[2], 3), 0, VOCAB - 1).astype(jnp.int32),
        "grammar_bits": draw_grammar_bits(jax.random.fold_in(splits[4], 71), 0),
    }


softcap = 30.0


def reference(hidden, embedding, targets, grammar_bits):
    row_count = hidden.shape[0]
    block_rows = math.gcd(row_count, 256)
    block_count = row_count // block_rows
    vocab_count = embedding.shape[0]
    vocab_ids = jnp.arange(vocab_count, dtype=jnp.int32)
    shifts = jnp.arange(32, dtype=jnp.int32)

    def one_block(running, inputs):
        hidden_block, target_block, bit_block = inputs
        scores = jnp.dot(hidden_block, embedding.T, preferred_element_type=jnp.float32)
        capped = softcap * jnp.tanh(scores / softcap)
        unpacked = jnp.right_shift(bit_block[:, :, None], shifts[None, None, :]) & 1
        unpacked = unpacked.reshape(block_rows, vocab_count)
        onehot = vocab_ids[None, :] == target_block[:, None]
        allowed = (unpacked == 1) | onehot
        totals = jnp.sum(jnp.where(allowed, jnp.exp(capped), 0.0), axis=1)
        log_total = jnp.log(totals)
        target_logit = jnp.sum(jnp.where(onehot, capped, 0.0), axis=1)
        block_loss = log_total - target_logit
        probability = jnp.where(allowed, jnp.exp(capped - log_total[:, None]), 0.0)
        softcap_slope = 1.0 - jnp.square(capped / softcap)
        dlogit = ((probability - onehot.astype(jnp.float32)) * softcap_slope).astype(jnp.bfloat16)
        block_hidden_grad = jnp.dot(dlogit, embedding, preferred_element_type=jnp.float32)
        running = running + jnp.dot(dlogit.T, hidden_block, preferred_element_type=jnp.float32)
        return running, (block_loss, block_hidden_grad)

    zero_grad = jnp.zeros((vocab_count, hidden.shape[1]), jnp.float32)
    embed_grad, (block_loss, block_hidden_grad) = lax.scan(
        one_block,
        zero_grad,
        (hidden.reshape(block_count, block_rows, hidden.shape[1]),
         targets.reshape(block_count, block_rows),
         grammar_bits.reshape(block_count, block_rows, grammar_bits.shape[1])))
    token_loss = block_loss.reshape(row_count)
    hidden_grad = block_hidden_grad.reshape(row_count, hidden.shape[1])
    return token_loss, hidden_grad, embed_grad
```

```python
import functools

import jax
import jax.numpy as jnp
from jax import lax
from jax.experimental import pallas as pl
from jax.experimental.pallas import tpu as pltpu
from jax.sharding import PartitionSpec as P

softcap = 30.0
MESH = pl.DeviceIdType.MESH
f32 = jnp.float32
bf16 = jnp.bfloat16


def kernel(
    data, outer, inner,
    hidden_hbm, embed_hbm, targets_hbm, bits_hbm,
    loss_ref, hgrad_ref, egrad_hbm,
    own, emb, tgt, bits, gath, cols, dl, h2, stat, stat_in,
    part, y_out, y_in, total, z_out, z_in, egrad, allow, hot,
    local_sem, emb_sem, place_sem, egrad_sem,
    gz_s, gz_r, gy_s, gy_r, gd_s, gd_r, st_s, st_r, dl_s, dl_r,
    ry_s, ry_r, rz_s, rz_r,
):
    d = lax.axis_index("dp")
    v = lax.axis_index("vocab")
    group = outer * inner
    a, b = v // inner, v % inner
    rows, width = own.shape[0], emb.shape[2]
    vocab_local = emb.shape[1]
    tokens = group * rows

    def at_outer(i):
        return ((a + i) % outer) * inner + b

    def at_inner(i):
        return a * inner + (b + i) % inner

    def columns(j):
        return pl.ds(pl.multiple_of(j * width, 128), width)

    def remote(src, dst, send, recv, **where):
        return pltpu.make_async_remote_copy(
            src_ref=src, dst_ref=dst, send_sem=send, recv_sem=recv,
            device_id=where, device_id_type=MESH,
        )

    order = [(d + 1 + k) % data for k in range(data)]
    own_copy = pltpu.make_async_copy(hidden_hbm, own, local_sem.at[0])
    own_copy.start()
    tgt_copy = pltpu.make_async_copy(targets_hbm, tgt, local_sem.at[1])
    tgt_copy.start()
    bits_copy = pltpu.make_async_copy(bits_hbm, bits, local_sem.at[2])
    bits_copy.start()
    barrier = pltpu.get_barrier_semaphore()
    for i in range(1, group):
        pl.semaphore_signal(barrier, inc=1, device_id={"vocab": (v + i) % group}, device_id_type=MESH)
    for i in range(1, data):
        pl.semaphore_signal(barrier, inc=1, device_id={"dp": (d + i) % data}, device_id_type=MESH)
    emb_copy = []
    for k in range(data):
        j = order[k]
        copy = pltpu.make_async_copy(embed_hbm.at[:, columns(j)], emb.at[j], emb_sem.at[k])
        copy.start()
        emb_copy.append(copy)
    own_copy.wait()
    pl.semaphore_wait(barrier, group - 1 + data - 1)

    pending = []
    gz, place = [], []
    for k in range(data):
        j = order[k]
        copy = pltpu.make_async_copy(own.at[:, columns(j)], gath.at[j, a, b], place_sem.at[k])
        copy.start()
        place.append(copy)
        hops = []
        for i in range(1, outer):
            copy = remote(
                own.at[:, columns(j)], gath.at[j, a, b], gz_s.at[k, i - 1], gz_r.at[k, i - 1],
                vocab=at_outer(i),
            )
            copy.start()
            hops.append(copy)
        gz.append(hops)
        pending += hops

    tgt_copy.wait()
    bits_copy.wait()
    row_id = lax.broadcasted_iota(jnp.int32, (tokens, tokens), 0)
    col_id = lax.broadcasted_iota(jnp.int32, (tokens, tokens), 1)
    eye = row_id == col_id

    def to_column(row):
        return jnp.sum(jnp.where(eye, jnp.broadcast_to(row, (tokens, tokens)), 0.0), axis=1, keepdims=True)

    def to_row(column):
        return jnp.sum(jnp.where(eye, jnp.broadcast_to(column, (tokens, tokens)), 0.0), axis=0, keepdims=True)

    target = to_column(tgt[...].astype(f32))
    lane = lax.broadcasted_iota(jnp.int32, (tokens, 128), 1)
    shift = lane & 31
    slot = lane // 32
    for tile in range(vocab_local // 128):
        word = jnp.broadcast_to(bits[:, 4 * tile:4 * tile + 1], (tokens, 128))
        for w in range(1, 4):
            piece = jnp.broadcast_to(bits[:, 4 * tile + w:4 * tile + w + 1], (tokens, 128))
            word = jnp.where(slot == w, piece, word)
        set_bit = lax.shift_right_arithmetic(word, shift) & 1
        ids = (lane + (v * vocab_local + tile * 128)).astype(f32)
        is_target = jnp.where(ids == target, 1.0, 0.0)
        span = slice(tile * 128, tile * 128 + 128)
        hot[:, span] = is_target
        allow[:, span] = jnp.maximum(set_bit.astype(f32), is_target)
    stat[...] = jnp.zeros(stat.shape, f32)

    gy = []
    for k in range(data):
        j = order[k]
        place[k].wait()
        for copy in gz[k]:
            copy.wait_recv()
        hops = []
        for i in range(1, inner):
            copy = remote(
                gath.at[j, :, b], gath.at[j, :, b], gy_s.at[k, i - 1], gy_r.at[k, i - 1],
                vocab=at_inner(i),
            )
            copy.start()
            hops.append(copy)
        gy.append(hops)
        pending += hops

    scores = jnp.zeros((tokens, vocab_local), f32)
    gd = []
    for k in range(data):
        j = order[k]
        for copy in gy[k]:
            copy.wait_recv()
        if k < data - 1:
            copy = remote(gath.at[j], cols.at[k], gd_s.at[k], gd_r.at[k], dp=j)
            copy.start()
            gd.append(copy)
            pending.append(copy)
        block = gath[j].astype(f32).reshape(tokens, width).astype(bf16)
        if k == data - 1:
            h2[data - 1] = block
        emb_copy[k].wait()
        scores += lax.dot_general(block, emb[j], (((1,), (1,)), ((), ())), preferred_element_type=f32)

    bent = jnp.tanh(scores / softcap)
    capped = softcap * bent
    hot_now = hot[...]
    weight = jnp.where(allow[...] > 0.0, jnp.exp(capped), 0.0)
    stat[0:1, 0:tokens] = to_row(jnp.sum(weight, axis=1, keepdims=True))
    stat[1:2, 0:tokens] = to_row(jnp.sum(hot_now * capped, axis=1, keepdims=True))
    st = []
    for i in range(1, group):
        copy = remote(stat, stat_in.at[i - 1], st_s.at[i - 1], st_r.at[i - 1], vocab=(v + i) % group)
        copy.start()
        st.append(copy)
    pending += st
    slope = 1.0 - jnp.square(bent)
    summed = stat[...]
    for i in range(1, group):
        st[i - 1].wait_recv()
        summed = summed + stat_in[i - 1]
    sums = summed[0:1, 0:tokens]
    loss_ref[...] = jnp.log(sums) - summed[1:2, 0:tokens]
    share = to_column(1.0 / sums)
    dlogit = ((weight * share - hot_now) * slope).astype(bf16)
    dl[data - 1] = dlogit

    dx, ry = [], []
    for k in range(data):
        part[k] = jnp.dot(dlogit, emb[k], preferred_element_type=f32).reshape(outer, inner, rows, width)
        hops = []
        for i in range(1, inner):
            mine = part[k, :, (b + i) % inner].reshape(outer * rows, width)
            y_out[k, i - 1] = mine.astype(bf16)
            copy = remote(
                y_out.at[k, i - 1], y_in.at[k, i - 1], ry_s.at[k, i - 1], ry_r.at[k, i - 1],
                vocab=at_inner(i),
            )
            copy.start()
            hops.append(copy)
        ry.append(hops)
        pending += hops
        if k == 0:
            for i in range(data - 1):
                copy = remote(
                    dl.at[data - 1], dl.at[i], dl_s.at[i], dl_r.at[i], dp=(d + 1 + i) % data
                )
                copy.start()
                dx.append(copy)
            pending += dx

    rz = []
    for k in range(data):
        now = part[k, :, b]
        for i in range(1, inner):
            ry[k][i - 1].wait_recv()
            now = now + y_in[k, i - 1].astype(f32).reshape(outer, rows, width)
        total[k] = now
        hops = []
        for i in range(1, outer):
            z_out[k, i - 1] = total[k, (a + i) % outer].astype(bf16)
            copy = remote(
                z_out.at[k, i - 1], z_in.at[k, i - 1], rz_s.at[k, i - 1], rz_r.at[k, i - 1],
                vocab=at_outer(i),
            )
            copy.start()
            hops.append(copy)
        rz.append(hops)
        pending += hops

    for k in range(data - 1):
        gd[k].wait_recv()
        h2[k] = cols[k].astype(f32).reshape(tokens, width).astype(bf16)
        dx[k].wait_recv()
    everything = h2[...].reshape(data * tokens, width)
    out_copies = []
    for tile in range(vocab_local // 128):
        span = slice(tile * 128, tile * 128 + 128)
        left = dl[:, :, span].reshape(data * tokens, 128)
        egrad[span, :] = lax.dot_general(
            left, everything, (((0,), (0,)), ((), ())), preferred_element_type=f32
        )
        copy = pltpu.make_async_copy(egrad.at[span], egrad_hbm.at[span], egrad_sem.at[tile])
        copy.start()
        out_copies.append(copy)

    for k in range(data):
        now = total[k, a]
        for i in range(1, outer):
            rz[k][i - 1].wait_recv()
            now = now + z_in[k, i - 1].astype(f32)
        hgrad_ref[:, k * width:(k + 1) * width] = now
    for copy in pending:
        copy.wait_send()
    for copy in out_copies:
        copy.wait()


def on_device(data, group, hidden, embedding, targets, grammar_bits):
    inner = 1 << ((group.bit_length() - 1) // 2)
    outer = group // inner
    rows, depth = hidden.shape
    vocab_local = embedding.shape[0]
    width = depth // data
    tokens = rows * group
    lanes = -(-tokens // 128) * 128
    more_in, more_out = max(inner - 1, 1), max(outer - 1, 1)
    dma = pltpu.SemaphoreType.DMA
    vmem = pltpu.VMEM
    anywhere = pl.BlockSpec(memory_space=pl.ANY)
    inside = pl.BlockSpec(memory_space=pltpu.VMEM)
    loss, hidden_grad, embed_grad = pl.pallas_call(
        functools.partial(kernel, data, outer, inner),
        out_shape=(
            jax.ShapeDtypeStruct((1, tokens), f32),
            jax.ShapeDtypeStruct((rows, depth), f32),
            jax.ShapeDtypeStruct((vocab_local, width), f32),
        ),
        in_specs=[anywhere] * 4,
        out_specs=(inside, inside, anywhere),
        scratch_shapes=[
            vmem((rows, depth), bf16),
            vmem((data, vocab_local, width), bf16),
            vmem((1, tokens), jnp.int32),
            vmem(grammar_bits.shape, jnp.int32),
            vmem((data, outer, inner, rows, width), bf16),
            vmem((data - 1, outer, inner, rows, width), bf16),
            vmem((data, tokens, vocab_local), bf16),
            vmem((data, tokens, width), bf16),
            vmem((2, lanes), f32),
            vmem((group - 1, 2, lanes), f32),
            vmem((data, outer, inner, rows, width), f32),
            vmem((data, more_in, outer * rows, width), bf16),
            vmem((data, more_in, outer * rows, width), bf16),
            vmem((data, outer, rows, width), f32),
            vmem((data, more_out, rows, width), bf16),
            vmem((data, more_out, rows, width), bf16),
            vmem((vocab_local, width), f32),
            vmem((tokens, vocab_local), f32),
            vmem((tokens, vocab_local), f32),
            dma((3,)), dma((data,)), dma((data,)), dma((vocab_local // 128,)),
            dma((data, more_out)), dma((data, more_out)),
            dma((data, more_in)), dma((data, more_in)),
            dma((data - 1,)), dma((data - 1,)),
            dma((group - 1,)), dma((group - 1,)),
            dma((data - 1,)), dma((data - 1,)),
            dma((data, more_in)), dma((data, more_in)),
            dma((data, more_out)), dma((data, more_out)),
        ],
        compiler_params=pltpu.CompilerParams(
            collective_id=0, has_side_effects=True, vmem_limit_bytes=60 * 2**20
        ),
    )(hidden, embedding, targets.reshape(1, tokens), grammar_bits)
    return loss.reshape(tokens), hidden_grad, embed_grad


def solution(mesh):
    in_specs = (P(("dp", "vocab"), None), P("vocab", None), P("dp"), P("dp", "vocab"))
    out_specs = (P("dp"), P(("dp", "vocab"), None), P("vocab", "dp"))
    body = functools.partial(on_device, mesh.shape["dp"], mesh.shape["vocab"])
    return jax.shard_map(body, mesh=mesh, in_specs=in_specs, out_specs=out_specs, check_vma=False)
```

```python
import functools

import jax
import jax.numpy as jnp
from jax import lax
from jax.experimental import pallas as pl
from jax.experimental.pallas import tpu as pltpu
from jax.sharding import PartitionSpec as P

softcap = 30.0
MESH = pl.DeviceIdType.MESH
f32 = jnp.float32
bf16 = jnp.bfloat16


def kernel(
    data, outer, inner,
    hidden_hbm, embed_hbm, targets_hbm, bits_hbm,
    loss_ref, hgrad_ref, egrad,
    own, emb, tgt, bits, gath, cols, dl, h2, stat, stat_in,
    part, y_out, y_in, total, z_out, z_in, allow, hot,
    local_sem, emb_sem, place_sem,
    gz_s, gz_r, gy_s, gy_r, gd_s, gd_r, st_s, st_r, dl_s, dl_r,
    ry_s, ry_r, rz_s, rz_r,
):
    d = lax.axis_index("dp")
    v = lax.axis_index("vocab")
    group = outer * inner
    a, b = v // inner, v % inner
    rows, width = own.shape[0], emb.shape[2]
    vocab_local = emb.shape[1]
    tokens = group * rows

    def at_outer(i):
        return ((a + i) % outer) * inner + b

    def at_inner(i):
        return a * inner + (b + i) % inner

    def columns(j):
        return pl.ds(pl.multiple_of(j * width, 128), width)

    def remote(src, dst, send, recv, **where):
        return pltpu.make_async_remote_copy(
            src_ref=src, dst_ref=dst, send_sem=send, recv_sem=recv,
            device_id=where, device_id_type=MESH,
        )

    order = [(d + 1 + k) % data for k in range(data)]
    own_copy = pltpu.make_async_copy(hidden_hbm, own, local_sem.at[0])
    own_copy.start()
    tgt_copy = pltpu.make_async_copy(targets_hbm, tgt, local_sem.at[1])
    tgt_copy.start()
    bits_copy = pltpu.make_async_copy(bits_hbm, bits, local_sem.at[2])
    bits_copy.start()
    barrier = pltpu.get_barrier_semaphore()
    for i in range(1, group):
        pl.semaphore_signal(barrier, inc=1, device_id={"vocab": (v + i) % group}, device_id_type=MESH)
    for i in range(1, data):
        pl.semaphore_signal(barrier, inc=1, device_id={"dp": (d + i) % data}, device_id_type=MESH)
    emb_copy = []
    for k in range(data):
        j = order[k]
        copy = pltpu.make_async_copy(embed_hbm.at[:, columns(j)], emb.at[j], emb_sem.at[k])
        copy.start()
        emb_copy.append(copy)
    own_copy.wait()
    pl.semaphore_wait(barrier, group - 1 + data - 1)

    pending = []
    gz, place = [], []
    for k in range(data):
        j = order[k]
        copy = pltpu.make_async_copy(own.at[:, columns(j)], gath.at[j, a, b], place_sem.at[k])
        copy.start()
        place.append(copy)
        hops = []
        for i in range(1, outer):
            copy = remote(
                own.at[:, columns(j)], gath.at[j, a, b], gz_s.at[k, i - 1], gz_r.at[k, i - 1],
                vocab=at_outer(i),
            )
            copy.start()
            hops.append(copy)
        gz.append(hops)
        pending += hops

    tgt_copy.wait()
    bits_copy.wait()
    row_id = lax.broadcasted_iota(jnp.int32, (tokens, tokens), 0)
    col_id = lax.broadcasted_iota(jnp.int32, (tokens, tokens), 1)
    eye = row_id == col_id

    def to_column(row):
        return jnp.sum(jnp.where(eye, jnp.broadcast_to(row, (tokens, tokens)), 0.0), axis=1, keepdims=True)

    def to_row(column):
        return jnp.sum(jnp.where(eye, jnp.broadcast_to(column, (tokens, tokens)), 0.0), axis=0, keepdims=True)

    target = to_column(tgt[...].astype(f32))
    lane = lax.broadcasted_iota(jnp.int32, (tokens, 128), 1)
    shift = lane & 31
    slot = lane // 32
    words = bits[...].T
    for tile in range(vocab_local // 128):
        word = jnp.broadcast_to(words[:, 4 * tile:4 * tile + 1], (tokens, 128))
        for w in range(1, 4):
            piece = jnp.broadcast_to(words[:, 4 * tile + w:4 * tile + w + 1], (tokens, 128))
            word = jnp.where(slot == w, piece, word)
        set_bit = lax.shift_right_arithmetic(word, shift) & 1
        ids = (lane + (v * vocab_local + tile * 128)).astype(f32)
        is_target = jnp.where(ids == target, 1.0, 0.0)
        span = slice(tile * 128, tile * 128 + 128)
        hot[:, span] = is_target
        allow[:, span] = jnp.maximum(set_bit.astype(f32), is_target)
    stat[...] = jnp.zeros(stat.shape, f32)

    gy = []
    for k in range(data):
        j = order[k]
        place[k].wait()
        for copy in gz[k]:
            copy.wait_recv()
        hops = []
        for i in range(1, inner):
            copy = remote(
                gath.at[j, :, b], gath.at[j, :, b], gy_s.at[k, i - 1], gy_r.at[k, i - 1],
                vocab=at_inner(i),
            )
            copy.start()
            hops.append(copy)
        gy.append(hops)
        pending += hops

    scores = jnp.zeros((tokens, vocab_local), f32)
    gd = []
    for k in range(data):
        j = order[k]
        for copy in gy[k]:
            copy.wait_recv()
        if k < data - 1:
            copy = remote(gath.at[j], cols.at[k], gd_s.at[k], gd_r.at[k], dp=j)
            copy.start()
            gd.append(copy)
            pending.append(copy)
        block = gath[j].astype(f32).reshape(tokens, width).astype(bf16)
        if k == data - 1:
            h2[data - 1] = block
        emb_copy[k].wait()
        scores += lax.dot_general(block, emb[j], (((1,), (1,)), ((), ())), preferred_element_type=f32)

    bent = jnp.tanh(scores / softcap)
    capped = softcap * bent
    hot_now = hot[...]
    weight = jnp.where(allow[...] > 0.0, jnp.exp(capped), 0.0)
    stat[0:1, 0:tokens] = to_row(jnp.sum(weight, axis=1, keepdims=True))
    stat[1:2, 0:tokens] = to_row(jnp.sum(hot_now * capped, axis=1, keepdims=True))
    st = []
    for i in range(1, group):
        copy = remote(stat, stat_in.at[i - 1], st_s.at[i - 1], st_r.at[i - 1], vocab=(v + i) % group)
        copy.start()
        st.append(copy)
    pending += st
    slope = 1.0 - jnp.square(bent)
    summed = stat[...]
    for i in range(1, group):
        st[i - 1].wait_recv()
        summed = summed + stat_in[i - 1]
    sums = summed[0:1, 0:tokens]
    loss_ref[...] = jnp.log(sums) - summed[1:2, 0:tokens]
    share = to_column(1.0 / sums)
    dlogit = ((weight * share - hot_now) * slope).astype(bf16)
    dl[data - 1] = dlogit

    dx, ry = [], []
    for k in range(data):
        part[k] = jnp.dot(dlogit, emb[k], preferred_element_type=f32).reshape(outer, inner, rows, width)
        hops = []
        for i in range(1, inner):
            mine = part[k, :, (b + i) % inner].reshape(outer * rows, width)
            y_out[k, i - 1] = mine.astype(bf16)
            copy = remote(
                y_out.at[k, i - 1], y_in.at[k, i - 1], ry_s.at[k, i - 1], ry_r.at[k, i - 1],
                vocab=at_inner(i),
            )
            copy.start()
            hops.append(copy)
        ry.append(hops)
        pending += hops
        if k == 0:
            for i in range(data - 1):
                copy = remote(
                    dl.at[data - 1], dl.at[i], dl_s.at[i], dl_r.at[i], dp=(d + 1 + i) % data
                )
                copy.start()
                dx.append(copy)
            pending += dx

    rz = []
    for k in range(data):
        now = part[k, :, b]
        for i in range(1, inner):
            ry[k][i - 1].wait_recv()
            now = now + y_in[k, i - 1].astype(f32).reshape(outer, rows, width)
        total[k] = now
        hops = []
        for i in range(1, outer):
            z_out[k, i - 1] = total[k, (a + i) % outer].astype(bf16)
            copy = remote(
                z_out.at[k, i - 1], z_in.at[k, i - 1], rz_s.at[k, i - 1], rz_r.at[k, i - 1],
                vocab=at_outer(i),
            )
            copy.start()
            hops.append(copy)
        rz.append(hops)
        pending += hops

    for k in range(data - 1):
        gd[k].wait_recv()
        h2[k] = cols[k].astype(f32).reshape(tokens, width).astype(bf16)
        dx[k].wait_recv()
    everything = h2[...].reshape(data * tokens, width)
    for tile in range(vocab_local // 128):
        span = slice(tile * 128, tile * 128 + 128)
        left = dl[:, :, span].reshape(data * tokens, 128)
        egrad[span, :] = lax.dot_general(
            left, everything, (((0,), (0,)), ((), ())), preferred_element_type=f32
        )

    for k in range(data):
        now = total[k, a]
        for i in range(1, outer):
            rz[k][i - 1].wait_recv()
            now = now + z_in[k, i - 1].astype(f32)
        hgrad_ref[:, k * width:(k + 1) * width] = now
    for copy in pending:
        copy.wait_send()


def write_out(loss, hgrad, egrad, loss_out, hgrad_out, egrad_out, sems):
    pairs = [(egrad, egrad_out), (hgrad, hgrad_out), (loss, loss_out)]
    copies = [pltpu.make_async_copy(src, dst, sems.at[i]) for i, (src, dst) in enumerate(pairs)]
    for copy in copies:
        copy.start()
    for copy in copies:
        copy.wait()


def on_device(data, group, hidden, embedding, targets, grammar_bits):
    inner = 1 << ((group.bit_length() - 1) // 2)
    outer = group // inner
    rows, depth = hidden.shape
    vocab_local = embedding.shape[0]
    width = depth // data
    tokens = rows * group
    lanes = -(-tokens // 128) * 128
    more_in, more_out = max(inner - 1, 1), max(outer - 1, 1)
    dma = pltpu.SemaphoreType.DMA
    vmem = pltpu.VMEM
    anywhere = pl.BlockSpec(memory_space=pltpu.HBM)
    inside = pl.BlockSpec(memory_space=pltpu.VMEM)
    operands = (hidden, embedding, targets.reshape(1, tokens), grammar_bits.T)
    loss, hidden_grad, embed_grad = pl.pallas_call(
        functools.partial(kernel, data, outer, inner),
        out_shape=(
            vmem((1, tokens), f32),
            vmem((rows, depth), f32),
            vmem((vocab_local, width), f32),
        ),
        in_specs=[anywhere] * 4,
        out_specs=(inside, inside, inside),
        scratch_shapes=[
            vmem((rows, depth), bf16),
            vmem((data, vocab_local, width), bf16),
            vmem((1, tokens), jnp.int32),
            vmem(grammar_bits.shape[::-1], jnp.int32),
            vmem((data, outer, inner, rows, width), bf16),
            vmem((data - 1, outer, inner, rows, width), bf16),
            vmem((data, tokens, vocab_local), bf16),
            vmem((data, tokens, width), bf16),
            vmem((2, lanes), f32),
            vmem((group - 1, 2, lanes), f32),
            vmem((data, outer, inner, rows, width), f32),
            vmem((data, more_in, outer * rows, width), bf16),
            vmem((data, more_in, outer * rows, width), bf16),
            vmem((data, outer, rows, width), f32),
            vmem((data, more_out, rows, width), bf16),
            vmem((data, more_out, rows, width), bf16),
            vmem((tokens, vocab_local), f32),
            vmem((tokens, vocab_local), f32),
            dma((3,)), dma((data,)), dma((data,)),
            dma((data, more_out)), dma((data, more_out)),
            dma((data, more_in)), dma((data, more_in)),
            dma((data - 1,)), dma((data - 1,)),
            dma((group - 1,)), dma((group - 1,)),
            dma((data - 1,)), dma((data - 1,)),
            dma((data, more_in)), dma((data, more_in)),
            dma((data, more_out)), dma((data, more_out)),
        ],
        compiler_params=pltpu.CompilerParams(
            collective_id=0, has_side_effects=True, vmem_limit_bytes=48 * 2**20
        ),
    )(*(pltpu.with_memory_space_constraint(x, pltpu.HBM) for x in operands))
    loss, hidden_grad, embed_grad = pl.pallas_call(
        write_out,
        out_shape=tuple(jax.ShapeDtypeStruct(x.shape, f32) for x in (loss, hidden_grad, embed_grad)),
        in_specs=[inside] * 3,
        out_specs=(anywhere,) * 3,
        scratch_shapes=[dma((3,))],
    )(*(pltpu.with_memory_space_constraint(x, pltpu.VMEM) for x in (loss, hidden_grad, embed_grad)))
    return loss.reshape(tokens), hidden_grad, embed_grad


def solution(mesh):
    in_specs = (P(("dp", "vocab"), None), P("vocab", None), P("dp"), P("dp", "vocab"))
    out_specs = (P("dp"), P(("dp", "vocab"), None), P("vocab", "dp"))
    body = functools.partial(on_device, mesh.shape["dp"], mesh.shape["vocab"])
    return jax.shard_map(body, mesh=mesh, in_specs=in_specs, out_specs=out_specs, check_vma=False)
```

```python
import functools

import jax
import jax.numpy as jnp
from jax import lax
from jax.experimental import pallas as pl
from jax.experimental.pallas import tpu as pltpu
from jax.sharding import PartitionSpec as P

softcap = 30.0
MESH = pl.DeviceIdType.MESH
f32 = jnp.float32
bf16 = jnp.bfloat16


def kernel(
    data, outer, inner,
    hidden_hbm, embed_hbm, targets_hbm, bits_hbm,
    loss_ref, hgrad_ref, egrad,
    own, emb, tgt, bits, gath, cols, dl, h2, stat, stat_in,
    part, y_out, y_in, total, z_out, z_in, allow, hot,
    local_sem, emb_sem, place_sem,
    gz_s, gz_r, go_s, go_r, gy_s, gy_r, gd_s, gd_r, st_s, st_r, dl_s, dl_r,
    ry_s, ry_r, rz_s, rz_r,
):
    d = lax.axis_index("dp")
    v = lax.axis_index("vocab")
    group = outer * inner
    a, b = v // inner, v % inner
    rows, width = own.shape[0], emb.shape[2]
    vocab_local = emb.shape[1]
    tokens = group * rows

    def at_outer(i):
        return ((a + i) % outer) * inner + b

    def at_inner(i):
        return a * inner + (b + i) % inner

    def columns(j):
        return pl.ds(pl.multiple_of(j * width, 128), width)

    def remote(src, dst, send, recv, **where):
        return pltpu.make_async_remote_copy(
            src_ref=src, dst_ref=dst, send_sem=send, recv_sem=recv,
            device_id=where, device_id_type=MESH,
        )

    order = [(d + 1 + k) % data for k in range(data)]
    own_copy = pltpu.make_async_copy(hidden_hbm, own, local_sem.at[0])
    own_copy.start()
    tgt_copy = pltpu.make_async_copy(targets_hbm, tgt, local_sem.at[1])
    tgt_copy.start()
    bits_copy = pltpu.make_async_copy(bits_hbm, bits, local_sem.at[2])
    bits_copy.start()
    barrier = pltpu.get_barrier_semaphore()
    for i in range(1, group):
        pl.semaphore_signal(barrier, inc=1, device_id={"vocab": (v + i) % group}, device_id_type=MESH)
    for i in range(1, data):
        pl.semaphore_signal(barrier, inc=1, device_id={"dp": (d + i) % data}, device_id_type=MESH)
    emb_copy = []
    for k in range(data):
        j = order[k]
        copy = pltpu.make_async_copy(embed_hbm.at[:, columns(j)], emb.at[j], emb_sem.at[k])
        copy.start()
        emb_copy.append(copy)
    own_copy.wait()
    pl.semaphore_wait(barrier, group - 1 + data - 1)

    half = (width // 128 + 1) // 2 * 128
    halves = [(0, half), (half, width - half)]
    pieces = [(k, h) for k in range(data) for h in range(2)]
    pending = []
    gz, go, place = [], [], []
    for k in range(data):
        j = order[k]
        copy = pltpu.make_async_copy(own.at[:, columns(j)], gath.at[j, 0, b], place_sem.at[k])
        copy.start()
        place.append(copy)
        for h in range(2):
            start, size = halves[h]
            source = own.at[:, pl.ds(pl.multiple_of(j * width + start, 128), size)]
            hops = []
            for i in range(1, outer):
                copy = remote(
                    source, gath.at[j, i, b, :, pl.ds(start, size)],
                    gz_s.at[2 * k + h, i - 1], gz_r.at[2 * k + h, i - 1], vocab=at_outer(i),
                )
                copy.start()
                hops.append(copy)
            gz.append(hops)
            pending += hops
        hops = []
        for i in range(1, inner):
            copy = remote(
                own.at[:, columns(j)], gath.at[j, 0, b], go_s.at[k, i - 1], go_r.at[k, i - 1],
                vocab=at_inner(i),
            )
            copy.start()
            hops.append(copy)
        go.append(hops)
        pending += hops

    tgt_copy.wait()
    bits_copy.wait()
    row_id = lax.broadcasted_iota(jnp.int32, (tokens, tokens), 0)
    col_id = lax.broadcasted_iota(jnp.int32, (tokens, tokens), 1)
    eye = row_id == col_id

    def to_column(row):
        return jnp.sum(jnp.where(eye, jnp.broadcast_to(row, (tokens, tokens)), 0.0), axis=1, keepdims=True)

    def to_row(column):
        return jnp.sum(jnp.where(eye, jnp.broadcast_to(column, (tokens, tokens)), 0.0), axis=0, keepdims=True)

    target = to_column(tgt[...].astype(f32))
    lane = lax.broadcasted_iota(jnp.int32, (tokens, 128), 1)
    shift = lane & 31
    slot = lane // 32
    words = bits[...].T
    for tile in range(vocab_local // 128):
        word = jnp.broadcast_to(words[:, 4 * tile:4 * tile + 1], (tokens, 128))
        for w in range(1, 4):
            piece = jnp.broadcast_to(words[:, 4 * tile + w:4 * tile + w + 1], (tokens, 128))
            word = jnp.where(slot == w, piece, word)
        set_bit = lax.shift_right_arithmetic(word, shift) & 1
        ids = (lane + (v * vocab_local + tile * 128)).astype(f32)
        is_target = jnp.where(ids == target, 1.0, 0.0)
        span = slice(tile * 128, tile * 128 + 128)
        hot[:, span] = is_target
        allow[:, span] = jnp.maximum(set_bit.astype(f32), is_target)
    stat[...] = jnp.zeros(stat.shape, f32)

    def in_order(block, span):
        found = [
            block[(a - i + outer) % outer, :, :, span].astype(f32).reshape(inner * rows, -1)
            for i in range(outer)
        ]
        return jnp.concatenate(found, axis=0).astype(bf16)

    gy, gd = [], []
    scores = jnp.zeros((tokens, vocab_local), f32)
    behind = 3
    for q in range(len(pieces) + behind):
        if q < len(pieces):
            k, h = pieces[q]
            span = pl.ds(*halves[h])
            for copy in gz[q]:
                copy.wait_recv()
            hops = []
            for i in range(1, inner):
                passed = gath.at[order[k], pl.ds(1, outer - 1), b, :, span]
                copy = remote(passed, passed, gy_s.at[q, i - 1], gy_r.at[q, i - 1], vocab=at_inner(i))
                copy.start()
                hops.append(copy)
            gy.append(hops)
            pending += hops
        if q >= behind:
            k, h = pieces[q - behind]
            j = order[k]
            start, size = halves[h]
            span = slice(start, start + size)
            if h == 0:
                place[k].wait()
                for copy in go[k]:
                    copy.wait_recv()
                emb_copy[k].wait()
            for copy in gy[q - behind]:
                copy.wait_recv()
            if h == 1 and k < data - 1:
                copy = remote(gath.at[j], cols.at[k], gd_s.at[k], gd_r.at[k], dp=j)
                copy.start()
                gd.append(copy)
                pending.append(copy)
            block = in_order(gath.at[j], span)
            if k == data - 1:
                h2[data - 1, :, span] = block
            scores += lax.dot_general(
                block, emb[j, :, span], (((1,), (1,)), ((), ())), preferred_element_type=f32
            )

    bent = jnp.tanh(scores / softcap)
    capped = softcap * bent
    hot_now = hot[...]
    weight = jnp.where(allow[...] > 0.0, jnp.exp(capped), 0.0)
    stat[0:1, 0:tokens] = to_row(jnp.sum(weight, axis=1, keepdims=True))
    stat[1:2, 0:tokens] = to_row(jnp.sum(hot_now * capped, axis=1, keepdims=True))
    st = []
    for i in range(1, group):
        copy = remote(stat, stat_in.at[i - 1], st_s.at[i - 1], st_r.at[i - 1], vocab=(v + i) % group)
        copy.start()
        st.append(copy)
    pending += st
    slope = 1.0 - jnp.square(bent)
    summed = stat[...]
    for i in range(1, group):
        st[i - 1].wait_recv()
        summed = summed + stat_in[i - 1]
    sums = summed[0:1, 0:tokens]
    loss_ref[...] = jnp.log(sums) - summed[1:2, 0:tokens]
    share = to_column(1.0 / sums)
    dlogit = ((weight * share - hot_now) * slope).astype(bf16)
    dl[data - 1] = dlogit

    dx, ry = [], []
    for q, (k, h) in enumerate(pieces):
        start, size = halves[h]
        span = slice(start, start + size)
        part[k, :, :, :, span] = jnp.dot(
            dlogit, emb[k, :, span], preferred_element_type=f32
        ).reshape(outer, inner, rows, size)
        hops = []
        for i in range(1, inner):
            mine = part[k, :, (b + i) % inner, :, span].reshape(outer * rows, size)
            y_out[k, i - 1, :, span] = mine.astype(bf16)
            copy = remote(
                y_out.at[k, i - 1, :, pl.ds(start, size)], y_in.at[k, i - 1, :, pl.ds(start, size)],
                ry_s.at[q, i - 1], ry_r.at[q, i - 1], vocab=at_inner(i),
            )
            copy.start()
            hops.append(copy)
        ry.append(hops)
        pending += hops
        if q == 0:
            for i in range(data - 1):
                copy = remote(
                    dl.at[data - 1], dl.at[i], dl_s.at[i], dl_r.at[i], dp=(d + 1 + i) % data
                )
                copy.start()
                dx.append(copy)
            pending += dx

    rz = []
    for q, (k, h) in enumerate(pieces):
        start, size = halves[h]
        span = slice(start, start + size)
        now = part[k, :, b, :, span]
        for i in range(1, inner):
            ry[q][i - 1].wait_recv()
            now = now + y_in[k, i - 1, :, span].astype(f32).reshape(outer, rows, size)
        total[k, :, :, span] = now
        hops = []
        for i in range(1, outer):
            z_out[k, i - 1, :, span] = total[k, (a + i) % outer, :, span].astype(bf16)
            copy = remote(
                z_out.at[k, i - 1, :, pl.ds(start, size)], z_in.at[k, i - 1, :, pl.ds(start, size)],
                rz_s.at[q, i - 1], rz_r.at[q, i - 1], vocab=at_outer(i),
            )
            copy.start()
            hops.append(copy)
        rz.append(hops)
        pending += hops

    for k in range(data - 1):
        gd[k].wait_recv()
        h2[k] = in_order(cols.at[k], slice(0, width))
        dx[k].wait_recv()
    everything = h2[...].reshape(data * tokens, width)
    for tile in range(vocab_local // 128):
        span = slice(tile * 128, tile * 128 + 128)
        left = dl[:, :, span].reshape(data * tokens, 128)
        egrad[span, :] = lax.dot_general(
            left, everything, (((0,), (0,)), ((), ())), preferred_element_type=f32
        )

    for q, (k, h) in enumerate(pieces):
        start, size = halves[h]
        span = slice(start, start + size)
        now = total[k, a, :, span]
        for i in range(1, outer):
            rz[q][i - 1].wait_recv()
            now = now + z_in[k, i - 1, :, span].astype(f32)
        hgrad_ref[:, k * width + start:k * width + start + size] = now
    for copy in pending:
        copy.wait_send()


def write_out(loss, hgrad, egrad, loss_out, hgrad_out, egrad_out, sems):
    pairs = [(egrad, egrad_out), (hgrad, hgrad_out), (loss, loss_out)]
    copies = [pltpu.make_async_copy(src, dst, sems.at[i]) for i, (src, dst) in enumerate(pairs)]
    for copy in copies:
        copy.start()
    for copy in copies:
        copy.wait()


def on_device(data, group, hidden, embedding, targets, grammar_bits):
    inner = 1 << ((group.bit_length() - 1) // 2)
    outer = group // inner
    rows, depth = hidden.shape
    vocab_local = embedding.shape[0]
    width = depth // data
    tokens = rows * group
    lanes = -(-tokens // 128) * 128
    more_in, more_out = max(inner - 1, 1), max(outer - 1, 1)
    dma = pltpu.SemaphoreType.DMA
    vmem = pltpu.VMEM
    anywhere = pl.BlockSpec(memory_space=pltpu.HBM)
    inside = pl.BlockSpec(memory_space=pltpu.VMEM)
    operands = (hidden, embedding, targets.reshape(1, tokens), grammar_bits.T)
    loss, hidden_grad, embed_grad = pl.pallas_call(
        functools.partial(kernel, data, outer, inner),
        out_shape=(
            vmem((1, tokens), f32),
            vmem((rows, depth), f32),
            vmem((vocab_local, width), f32),
        ),
        in_specs=[anywhere] * 4,
        out_specs=(inside, inside, inside),
        scratch_shapes=[
            vmem((rows, depth), bf16),
            vmem((data, vocab_local, width), bf16),
            vmem((1, tokens), jnp.int32),
            vmem(grammar_bits.shape[::-1], jnp.int32),
            vmem((data, outer, inner, rows, width), bf16),
            vmem((data - 1, outer, inner, rows, width), bf16),
            vmem((data, tokens, vocab_local), bf16),
            vmem((data, tokens, width), bf16),
            vmem((2, lanes), f32),
            vmem((group - 1, 2, lanes), f32),
            vmem((data, outer, inner, rows, width), f32),
            vmem((data, more_in, outer * rows, width), bf16),
            vmem((data, more_in, outer * rows, width), bf16),
            vmem((data, outer, rows, width), f32),
            vmem((data, more_out, rows, width), bf16),
            vmem((data, more_out, rows, width), bf16),
            vmem((tokens, vocab_local), f32),
            vmem((tokens, vocab_local), f32),
            dma((3,)), dma((data,)), dma((data,)),
            dma((2 * data, more_out)), dma((2 * data, more_out)),
            dma((data, more_in)), dma((data, more_in)),
            dma((2 * data, more_in)), dma((2 * data, more_in)),
            dma((data - 1,)), dma((data - 1,)),
            dma((group - 1,)), dma((group - 1,)),
            dma((data - 1,)), dma((data - 1,)),
            dma((2 * data, more_in)), dma((2 * data, more_in)),
            dma((2 * data, more_out)), dma((2 * data, more_out)),
        ],
        compiler_params=pltpu.CompilerParams(
            collective_id=0, has_side_effects=True, vmem_limit_bytes=48 * 2**20
        ),
    )(*(pltpu.with_memory_space_constraint(x, pltpu.HBM) for x in operands))
    loss, hidden_grad, embed_grad = pl.pallas_call(
        write_out,
        out_shape=tuple(jax.ShapeDtypeStruct(x.shape, f32) for x in (loss, hidden_grad, embed_grad)),
        in_specs=[inside] * 3,
        out_specs=(anywhere,) * 3,
        scratch_shapes=[dma((3,))],
    )(*(pltpu.with_memory_space_constraint(x, pltpu.VMEM) for x in (loss, hidden_grad, embed_grad)))
    return loss.reshape(tokens), hidden_grad, embed_grad


def solution(mesh):
    in_specs = (P(("dp", "vocab"), None), P("vocab", None), P("dp"), P("dp", "vocab"))
    out_specs = (P("dp"), P(("dp", "vocab"), None), P("vocab", "dp"))
    body = functools.partial(on_device, mesh.shape["dp"], mesh.shape["vocab"])
    return jax.shard_map(body, mesh=mesh, in_specs=in_specs, out_specs=out_specs, check_vma=False)
```

```python
import functools

import jax
import jax.numpy as jnp
from jax import lax
from jax.experimental import pallas as pl
from jax.experimental.pallas import tpu as pltpu
from jax.sharding import PartitionSpec as P

softcap = 30.0
MESH = pl.DeviceIdType.MESH
f32 = jnp.float32
bf16 = jnp.bfloat16


def kernel(
    data, outer, inner,
    hidden_hbm, embed_hbm, targets_hbm, bits_hbm,
    loss_ref, hgrad_ref, egrad,
    own, emb, tgt, bits, gath, cols, dl, h2, stat, stat_in,
    part, y_out, y_in, total, z_out, z_in, allow, hot,
    local_sem, emb_sem, place_sem,
    gz_s, gz_r, gy_s, gy_r, gd_s, gd_r, st_s, st_r, dl_s, dl_r,
    ry_s, ry_r, rz_s, rz_r,
):
    d = lax.axis_index("dp")
    v = lax.axis_index("vocab")
    group = outer * inner
    a, b = v // inner, v % inner
    rows, width = own.shape[0], emb.shape[2]
    vocab_local = emb.shape[1]
    tokens = group * rows

    def at_outer(i):
        return ((a + i) % outer) * inner + b

    def at_inner(i):
        return a * inner + (b + i) % inner

    def columns(j):
        return pl.ds(pl.multiple_of(j * width, 128), width)

    def remote(src, dst, send, recv, **where):
        return pltpu.make_async_remote_copy(
            src_ref=src, dst_ref=dst, send_sem=send, recv_sem=recv,
            device_id=where, device_id_type=MESH,
        )

    order = [(d + 1 + k) % data for k in range(data)]
    own_copy = pltpu.make_async_copy(hidden_hbm, own, local_sem.at[0])
    own_copy.start()
    tgt_copy = pltpu.make_async_copy(targets_hbm, tgt, local_sem.at[1])
    tgt_copy.start()
    bits_copy = pltpu.make_async_copy(bits_hbm, bits, local_sem.at[2])
    bits_copy.start()
    barrier = pltpu.get_barrier_semaphore()
    for i in range(1, group):
        pl.semaphore_signal(barrier, inc=1, device_id={"vocab": (v + i) % group}, device_id_type=MESH)
    for i in range(1, data):
        pl.semaphore_signal(barrier, inc=1, device_id={"dp": (d + i) % data}, device_id_type=MESH)
    emb_copy = []
    for k in range(data):
        j = order[k]
        copy = pltpu.make_async_copy(embed_hbm.at[:, columns(j)], emb.at[j], emb_sem.at[k])
        copy.start()
        emb_copy.append(copy)
    own_copy.wait()
    pl.semaphore_wait(barrier, group - 1 + data - 1)

    pending = []
    gz, place = [], []
    for k in range(data):
        j = order[k]
        copy = pltpu.make_async_copy(own.at[:, columns(j)], gath.at[j, a, b], place_sem.at[k])
        copy.start()
        place.append(copy)
        hops = []
        for i in range(1, outer):
            copy = remote(
                own.at[:, columns(j)], gath.at[j, a, b], gz_s.at[k, i - 1], gz_r.at[k, i - 1],
                vocab=at_outer(i),
            )
            copy.start()
            hops.append(copy)
        gz.append(hops)
        pending += hops

    tgt_copy.wait()
    bits_copy.wait()
    row_id = lax.broadcasted_iota(jnp.int32, (tokens, tokens), 0)
    col_id = lax.broadcasted_iota(jnp.int32, (tokens, tokens), 1)
    eye = row_id == col_id

    def to_column(row):
        return jnp.sum(jnp.where(eye, jnp.broadcast_to(row, (tokens, tokens)), 0.0), axis=1, keepdims=True)

    def to_row(column):
        return jnp.sum(jnp.where(eye, jnp.broadcast_to(column, (tokens, tokens)), 0.0), axis=0, keepdims=True)

    target = to_column(tgt[...].astype(f32))
    lane = lax.broadcasted_iota(jnp.int32, (tokens, 128), 1)
    shift = lane & 31
    slot = lane // 32
    words = bits[...].T
    for tile in range(vocab_local // 128):
        word = jnp.broadcast_to(words[:, 4 * tile:4 * tile + 1], (tokens, 128))
        for w in range(1, 4):
            piece = jnp.broadcast_to(words[:, 4 * tile + w:4 * tile + w + 1], (tokens, 128))
            word = jnp.where(slot == w, piece, word)
        set_bit = lax.shift_right_arithmetic(word, shift) & 1
        ids = (lane + (v * vocab_local + tile * 128)).astype(f32)
        is_target = jnp.where(ids == target, 1.0, 0.0)
        span = slice(tile * 128, tile * 128 + 128)
        hot[:, span] = is_target
        allow[:, span] = jnp.maximum(set_bit.astype(f32), is_target)
    stat[...] = jnp.zeros(stat.shape, f32)

    gy, gd = [], []
    scores = jnp.zeros((tokens, vocab_local), f32)
    behind = 2
    for step in range(data + behind):
        if step < data:
            k, j = step, order[step]
            place[k].wait()
            for copy in gz[k]:
                copy.wait_recv()
            hops = []
            for i in range(1, inner):
                copy = remote(
                    gath.at[j, :, b], gath.at[j, :, b], gy_s.at[k, i - 1], gy_r.at[k, i - 1],
                    vocab=at_inner(i),
                )
                copy.start()
                hops.append(copy)
            gy.append(hops)
            pending += hops
        if step >= behind:
            k, j = step - behind, order[step - behind]
            for copy in gy[k]:
                copy.wait_recv()
            if k < data - 1:
                copy = remote(gath.at[j], cols.at[k], gd_s.at[k], gd_r.at[k], dp=j)
                copy.start()
                gd.append(copy)
                pending.append(copy)
            block = gath[j].astype(f32).reshape(tokens, width).astype(bf16)
            if k == data - 1:
                h2[data - 1] = block
            emb_copy[k].wait()
            scores += lax.dot_general(
                block, emb[j], (((1,), (1,)), ((), ())), preferred_element_type=f32
            )

    bent = jnp.tanh(scores / softcap)
    capped = softcap * bent
    hot_now = hot[...]
    weight = jnp.where(allow[...] > 0.0, jnp.exp(capped), 0.0)
    stat[0:1, 0:tokens] = to_row(jnp.sum(weight, axis=1, keepdims=True))
    stat[1:2, 0:tokens] = to_row(jnp.sum(hot_now * capped, axis=1, keepdims=True))
    st = []
    for i in range(1, group):
        copy = remote(stat, stat_in.at[i - 1], st_s.at[i - 1], st_r.at[i - 1], vocab=(v + i) % group)
        copy.start()
        st.append(copy)
    pending += st
    slope = 1.0 - jnp.square(bent)
    summed = stat[...]
    for i in range(1, group):
        st[i - 1].wait_recv()
        summed = summed + stat_in[i - 1]
    sums = summed[0:1, 0:tokens]
    loss_ref[...] = jnp.log(sums) - summed[1:2, 0:tokens]
    share = to_column(1.0 / sums)
    dlogit = ((weight * share - hot_now) * slope).astype(bf16)
    dl[data - 1] = dlogit

    dx, ry = [], []
    for k in range(data):
        part[k] = jnp.dot(dlogit, emb[k], preferred_element_type=f32).reshape(outer, inner, rows, width)
        hops = []
        for i in range(1, inner):
            mine = part[k, :, (b + i) % inner].reshape(outer * rows, width)
            y_out[k, i - 1] = mine.astype(bf16)
            copy = remote(
                y_out.at[k, i - 1], y_in.at[k, i - 1], ry_s.at[k, i - 1], ry_r.at[k, i - 1],
                vocab=at_inner(i),
            )
            copy.start()
            hops.append(copy)
        ry.append(hops)
        pending += hops
        if k == 0:
            for i in range(data - 1):
                copy = remote(
                    dl.at[data - 1], dl.at[i], dl_s.at[i], dl_r.at[i], dp=(d + 1 + i) % data
                )
                copy.start()
                dx.append(copy)
            pending += dx

    rz = []
    for k in range(data):
        now = part[k, :, b]
        for i in range(1, inner):
            ry[k][i - 1].wait_recv()
            now = now + y_in[k, i - 1].astype(f32).reshape(outer, rows, width)
        total[k] = now
        hops = []
        for i in range(1, outer):
            z_out[k, i - 1] = total[k, (a + i) % outer].astype(bf16)
            copy = remote(
                z_out.at[k, i - 1], z_in.at[k, i - 1], rz_s.at[k, i - 1], rz_r.at[k, i - 1],
                vocab=at_outer(i),
            )
            copy.start()
            hops.append(copy)
        rz.append(hops)
        pending += hops

    for k in range(data - 1):
        gd[k].wait_recv()
        h2[k] = cols[k].astype(f32).reshape(tokens, width).astype(bf16)
        dx[k].wait_recv()
    everything = h2[...].reshape(data * tokens, width)

    @pl.loop(0, vocab_local // 128)
    def _(tile):
        span = pl.ds(pl.multiple_of(tile * 128, 128), 128)
        left = dl[:, :, span].reshape(data * tokens, 128)
        egrad[span, :] = lax.dot_general(
            left, everything, (((0,), (0,)), ((), ())), preferred_element_type=f32
        )

    for k in range(data):
        now = total[k, a]
        for i in range(1, outer):
            rz[k][i - 1].wait_recv()
            now = now + z_in[k, i - 1].astype(f32)
        hgrad_ref[:, k * width:(k + 1) * width] = now
    for copy in pending:
        copy.wait_send()


def write_out(loss, hgrad, egrad, loss_out, hgrad_out, egrad_out, sems):
    pairs = [(egrad, egrad_out), (hgrad, hgrad_out), (loss, loss_out)]
    copies = [pltpu.make_async_copy(src, dst, sems.at[i]) for i, (src, dst) in enumerate(pairs)]
    for copy in copies:
        copy.start()
    for copy in copies:
        copy.wait()


def on_device(data, group, hidden, embedding, targets, grammar_bits):
    inner = 1 << ((group.bit_length() - 1) // 2)
    outer = group // inner
    rows, depth = hidden.shape
    vocab_local = embedding.shape[0]
    width = depth // data
    tokens = rows * group
    lanes = -(-tokens // 128) * 128
    more_in, more_out = max(inner - 1, 1), max(outer - 1, 1)
    dma = pltpu.SemaphoreType.DMA
    vmem = pltpu.VMEM
    anywhere = pl.BlockSpec(memory_space=pltpu.HBM)
    inside = pl.BlockSpec(memory_space=pltpu.VMEM)
    operands = (hidden, embedding, targets.reshape(1, tokens), grammar_bits.T)
    loss, hidden_grad, embed_grad = pl.pallas_call(
        functools.partial(kernel, data, outer, inner),
        out_shape=(
            vmem((1, tokens), f32),
            vmem((rows, depth), f32),
            vmem((vocab_local, width), f32),
        ),
        in_specs=[anywhere] * 4,
        out_specs=(inside, inside, inside),
        scratch_shapes=[
            vmem((rows, depth), bf16),
            vmem((data, vocab_local, width), bf16),
            vmem((1, tokens), jnp.int32),
            vmem(grammar_bits.shape[::-1], jnp.int32),
            vmem((data, outer, inner, rows, width), bf16),
            vmem((data - 1, outer, inner, rows, width), bf16),
            vmem((data, tokens, vocab_local), bf16),
            vmem((data, tokens, width), bf16),
            vmem((2, lanes), f32),
            vmem((group - 1, 2, lanes), f32),
            vmem((data, outer, inner, rows, width), f32),
            vmem((data, more_in, outer * rows, width), bf16),
            vmem((data, more_in, outer * rows, width), bf16),
            vmem((data, outer, rows, width), f32),
            vmem((data, more_out, rows, width), bf16),
            vmem((data, more_out, rows, width), bf16),
            vmem((tokens, vocab_local), f32),
            vmem((tokens, vocab_local), f32),
            dma((3,)), dma((data,)), dma((data,)),
            dma((data, more_out)), dma((data, more_out)),
            dma((data, more_in)), dma((data, more_in)),
            dma((data - 1,)), dma((data - 1,)),
            dma((group - 1,)), dma((group - 1,)),
            dma((data - 1,)), dma((data - 1,)),
            dma((data, more_in)), dma((data, more_in)),
            dma((data, more_out)), dma((data, more_out)),
        ],
        compiler_params=pltpu.CompilerParams(
            collective_id=0, has_side_effects=True, vmem_limit_bytes=48 * 2**20
        ),
    )(*(pltpu.with_memory_space_constraint(x, pltpu.HBM) for x in operands))
    loss, hidden_grad, embed_grad = pl.pallas_call(
        write_out,
        out_shape=tuple(jax.ShapeDtypeStruct(x.shape, f32) for x in (loss, hidden_grad, embed_grad)),
        in_specs=[inside] * 3,
        out_specs=(anywhere,) * 3,
        scratch_shapes=[dma((3,))],
    )(*(pltpu.with_memory_space_constraint(x, pltpu.VMEM) for x in (loss, hidden_grad, embed_grad)))
    return loss.reshape(tokens), hidden_grad, embed_grad


def solution(mesh):
    in_specs = (P(("dp", "vocab"), None), P("vocab", None), P("dp"), P("dp", "vocab"))
    out_specs = (P("dp"), P(("dp", "vocab"), None), P("vocab", "dp"))
    body = functools.partial(on_device, mesh.shape["dp"], mesh.shape["vocab"])
    return jax.shard_map(body, mesh=mesh, in_specs=in_specs, out_specs=out_specs, check_vma=False)
```
